256 devices in a mesh: row: 4 (over x), col: 2 (over core), dp: 32 (over z, y).
Axes of the slice: x: 4, y: 4, z: 8, core: 2. Of those that a mesh axis runs over, the one named last changes fastest.
Arguments:
- out_grad: bfloat16 [32, 128, 4096], P('dp', 'col', 'row'), may hold values from -6 to 6
- saved_hidden: bfloat16 [32, 128, 14336], P('dp', 'row', 'col'), may hold values from -6 to 6
- down_weight: bfloat16 [14336, 4096], P(('col', 'dp'), 'row'), may hold values from -0.046875 to 0.046875
Outputs:
- hidden_grad: bfloat16 [32, 128, 14336], P('dp', 'row', 'col')
- weight_grad: bfloat16 [14336, 4096], P(('col', 'dp'), 'row')
The draws below stay inside these ranges and needn't reach their ends.
All inputs are finite; a program needn't handle non-finite values.
Results may differ from the reference program's by a relative error of at most 0.009.
Values may be sent and summed in bfloat16 or wider, within the bound.
No kernel may reach another device: no remote copies, remote signals or barrier semaphores. Data moves between devices by JAX's collectives and lax.ppermute only.
A program may use at most 64 MiB of HBM per device.

```python
import jax
import jax.numpy as jnp
from jax import lax

D = 4096
FF = 14336
TOK_REP = 128
REPLICAS = 32
N_ROW = 4


def levels(key, shape, split, least, high):
    loudness = 1.0
    for dim, shards_of in split:
        heights = jax.random.uniform(jax.random.fold_in(jax.random.fold_in(key, 6), dim), (shards_of,), jnp.float32, least / len(split), high / len(split))
        loudness = loudness * jnp.repeat(jnp.exp(heights), shape[dim] // shards_of).reshape((-1,) + (1,) * (len(shape) - 1 - dim))
    return loudness


def bell_draw(rng, shape, deviation, reach, shards=(), kind=jnp.bfloat16):
    entries = deviation * jax.random.normal(rng, shape, jnp.float32)
    if shards:
        entries = entries * levels(rng, shape, shards, -0.22, 0.18)
    return jnp.clip(entries, -reach, reach).astype(kind)


def setup_inputs(seed: int = 0) -> dict:
    seeds = jax.random.split(jax.random.key(seed), 4)
    return {
        "out_grad": bell_draw(seeds[0], (REPLICAS, TOK_REP, D), 1.0, 6.0, ((0, 32), (1, 2), (2, 4))),
        "saved_hidden": bell_draw(seeds[1], (REPLICAS, TOK_REP, FF), 1.0, 6.0, ((0, 32), (1, 4), (2, 2))),
        "down_weight": bell_draw(seeds[2], (FF, D), FF ** -0.5, 0.046875, ((0, 64), (1, 4))),
    }


def reference(out_grad, saved_hidden, down_weight):
    width = D // N_ROW
    flat_grad = out_grad.reshape(REPLICAS * TOK_REP, D)
    flat_hidden = saved_hidden.reshape(REPLICAS * TOK_REP, FF)
    accum = jnp.zeros((REPLICAS * TOK_REP, FF), jnp.float32)
    for block in range(N_ROW):
        left = flat_grad[:, block * width:(block + 1) * width]
        right = down_weight[:, block * width:(block + 1) * width]
        partial_term = lax.dot_general(left, right, (((1,), (1,)), ((), ())), preferred_element_type=jnp.float32)
        rounded = lax.optimization_barrier(partial_term.astype(jnp.bfloat16))
        accum = accum + rounded.astype(jnp.float32)
    hidden_grad = accum.astype(jnp.bfloat16).reshape(REPLICAS, TOK_REP, FF)
    total = lax.dot_general(flat_hidden, flat_grad, (((0,), (0,)), ((), ())), preferred_element_type=jnp.float32)
    factor = jnp.float32(1.0) / jnp.sqrt(jnp.float32(REPLICAS * TOK_REP))
    weight_grad = (total * factor).astype(jnp.bfloat16)
    return (hidden_grad, weight_grad)
```

```python
import jax
import jax.numpy as jnp
from jax import lax
from jax.sharding import Mesh
from jax.sharding import PartitionSpec as P

DP = ("z", "y")
COL_DP = ("col", "z", "y")


def shifted(value, axis, by):
    devices = lax.axis_size(axis)
    return lax.ppermute(value, axis, [(i, (i + by) % devices) for i in range(devices)])


def ring_parts(value, axis):
    devices = lax.axis_size(axis)
    half = value.shape[0] // 2
    out = [(0, 0, value)]
    ahead = back = value
    for step in range(1, devices // 2):
        ahead, back = shifted(ahead, axis, 1), shifted(back, axis, -1)
        out += [(-step, 0, ahead), (step, 0, back)]
    far = devices // 2
    return out + [(far, 0, shifted(ahead[:half], axis, 1)), (far, half, shifted(back[half:], axis, -1))]


def on_device(out_grad, saved_hidden, down_weight):
    rows, cols, zs, ys = (lax.axis_size(a) for a in ("row", "col", "z", "y"))
    row, col, z, y = (lax.axis_index(a) for a in ("row", "col", "z", "y"))
    grad, hidden = out_grad[0], saved_hidden[0]
    units, width = down_weight.shape
    tokens, wide = hidden.shape
    block = wide // zs
    f32 = jnp.float32

    own = jnp.zeros((zs, *grad.shape), grad.dtype)
    for distance, start, part in ring_parts(grad, "z"):
        own = lax.dynamic_update_slice(own, part[None], ((z + distance) % zs, start, 0))
    other = shifted(own, "col", 1)
    per_core = rows // cols
    by_row = lambda v: jnp.swapaxes(v.reshape(zs, per_core, tokens, width), 0, 1)
    pair = jnp.concatenate([by_row(own), by_row(other)])
    turn = (row - per_core * col) % rows
    grads = jnp.concatenate([pair, pair])
    grads = lax.dynamic_slice_in_dim(grads, turn, rows, 0).reshape(rows, zs * tokens, width)

    weight = jnp.zeros((ys * units, width), down_weight.dtype)
    for distance, start, part in ring_parts(down_weight, "y"):
        weight = lax.dynamic_update_slice(weight, part, ((y + distance) % ys * units + start, 0))

    mine = jnp.swapaxes(hidden.reshape(tokens, zs, block), 0, 1)
    mine = lax.all_to_all(mine, "z", 0, 0, tiled=True).reshape(zs * tokens, block)
    hiddens = jnp.concatenate([mine] + [shifted(mine, "row", -s) for s in range(1, rows)])

    def partial(s):
        return lax.dot_general(grads[s], weight, (((1,), (1,)), ((), ())), preferred_element_type=f32)

    summed = sum(shifted(partial(s).astype(jnp.bfloat16), "row", s).astype(f32) for s in range(1, rows)) + partial(0)
    local = summed.astype(jnp.bfloat16).reshape(zs, tokens, block)
    returned = lax.all_to_all(local, "z", 0, 0, tiled=True)
    hidden_grad = jnp.swapaxes(returned, 0, 1).reshape(1, tokens, wide)

    factor = f32(1.0) / jnp.sqrt(f32(rows * tokens * zs * ys))
    total = lax.dot_general(
        hiddens, grads.reshape(-1, width), (((0,), (0,)), ((), ())), preferred_element_type=f32
    ).astype(jnp.bfloat16)
    take = lambda s: lax.dynamic_slice_in_dim(total, (y + s) % ys * units, units, 0)
    added = take(0).astype(f32) + sum(shifted(take(s), "y", s).astype(f32) for s in range(1, ys))
    weight_grad = (added * factor).astype(jnp.bfloat16)
    return (hidden_grad, weight_grad)


def solution(mesh):
    dp = mesh.shape["dp"]
    split = Mesh(
        mesh.devices.reshape(mesh.shape["row"], mesh.shape["col"], 8, dp // 8),
        ("row", "col", "z", "y"),
    )
    in_specs = (P(DP, "col", "row"), P(DP, "row", "col"), P(COL_DP, "row"))
    out_specs = (P(DP, "row", "col"), P(COL_DP, "row"))
    return jax.shard_map(
        on_device, mesh=split, in_specs=in_specs, out_specs=out_specs, check_vma=False
    )
```

```python
import jax
import jax.numpy as jnp
from jax import lax
from jax.sharding import Mesh
from jax.sharding import PartitionSpec as P

DP = ("z", "y")
COL_DP = ("col", "z", "y")


def shifted(value, axis, by):
    devices = lax.axis_size(axis)
    return lax.ppermute(value, axis, [(i, (i + by) % devices) for i in range(devices)])


def direct_parts(value, axis):
    devices = lax.axis_size(axis)
    return [(0, 0, value)] + [(s, 0, shifted(value, axis, -s)) for s in range(1, devices)]


def ring_parts(value, axis):
    devices = lax.axis_size(axis)
    half = value.shape[0] // 2
    out = [(0, 0, value)]
    ahead = back = value
    far = devices // 2
    for step in range(1, far):
        ahead, back = shifted(ahead, axis, 1), shifted(back, axis, -1)
        out += [(-step, 0, ahead), (step, 0, back)]
    first = shifted(ahead[:half], axis, 1)
    second = shifted(back[half:], axis, -1)
    return out + [(far, 0, first), (far, half, second)]


def direct_sum(part, axis):
    devices = lax.axis_size(axis)
    f32 = jnp.float32
    sent = [shifted(part(s).astype(jnp.bfloat16), axis, s) for s in range(1, devices)]
    return part(0).astype(f32) + sum(v.astype(f32) for v in sent)


def ring_sum(part, axis):
    f32, bf16 = jnp.float32, jnp.bfloat16
    far, ahead, back = part(2), part(1), part(3)
    half = far.shape[0] // 2
    far_p = shifted(far[:half].astype(bf16), axis, 1)
    far_m = shifted(far[half:].astype(bf16), axis, -1)
    low_p = shifted(ahead[half:].astype(bf16), axis, 1)
    low_m = shifted(back[:half].astype(bf16), axis, -1)
    high_p = shifted((ahead[:half].astype(f32) + far_p.astype(f32)).astype(bf16), axis, 1)
    high_m = shifted((back[half:].astype(f32) + far_m.astype(f32)).astype(bf16), axis, -1)
    here = part(0).astype(f32)
    top = here[:half] + high_p.astype(f32) + low_m.astype(f32)
    bottom = here[half:] + low_p.astype(f32) + high_m.astype(f32)
    return jnp.concatenate([top, bottom])


def on_device(out_grad, saved_hidden, down_weight):
    rows, cols, zs, ys = (lax.axis_size(a) for a in ("row", "col", "z", "y"))
    row, col, z, y = (lax.axis_index(a) for a in ("row", "col", "z", "y"))
    grad, hidden = out_grad[0], saved_hidden[0]
    units, width = down_weight.shape
    tokens, wide = hidden.shape
    block = ys * units
    f32, bf16 = jnp.float32, jnp.bfloat16

    parts = direct_parts(down_weight, "y")
    weight = jnp.zeros((block, width), down_weight.dtype)
    for distance, start, part in parts:
        weight = lax.dynamic_update_slice(weight, part, ((y + distance) % ys * units + start, 0))

    mine = jnp.swapaxes(hidden.reshape(tokens, zs, block), 0, 1)
    mine = lax.all_to_all(mine, "z", 0, 0, tiled=True).reshape(zs * tokens, block)

    own = jnp.zeros((zs, *grad.shape), grad.dtype)
    for distance, start, part in ring_parts(grad, "z"):
        own = lax.dynamic_update_slice(own, part[None], ((z + distance) % zs, start, 0))
    other = shifted(own, "col", 1)
    per_core = rows // cols
    by_row = lambda v: jnp.swapaxes(v.reshape(zs, per_core, tokens, width), 0, 1)
    pair = jnp.concatenate([by_row(own), by_row(other)])
    turn = (row - per_core * col) % rows
    grads = jnp.concatenate([pair, pair])
    grads = lax.dynamic_slice_in_dim(grads, turn, rows, 0).reshape(rows, zs * tokens, width)

    parts = direct_parts(mine, "row")
    hiddens = jnp.concatenate([part for _, _, part in parts])

    def partial(s):
        return lax.dot_general(grads[s], weight, (((1,), (1,)), ((), ())), preferred_element_type=f32)

    local = ring_sum(partial, "row").astype(bf16).reshape(zs, tokens, block)
    returned = lax.all_to_all(local, "z", 0, 0, tiled=True)
    hidden_grad = jnp.swapaxes(returned, 0, 1).reshape(1, tokens, wide)

    factor = f32(1.0) / jnp.sqrt(f32(rows * tokens * zs * ys))
    total = lax.dot_general(
        hiddens, grads.reshape(-1, width), (((0,), (0,)), ((), ())), preferred_element_type=f32
    ).astype(bf16)
    take = lambda s: lax.dynamic_slice_in_dim(total, (y + s) % ys * units, units, 0)
    weight_grad = (direct_sum(take, "y") * factor).astype(bf16)
    return (hidden_grad, weight_grad)


def solution(mesh):
    dp = mesh.shape["dp"]
    split = Mesh(
        mesh.devices.reshape(mesh.shape["row"], mesh.shape["col"], 8, dp // 8),
        ("row", "col", "z", "y"),
    )
    in_specs = (P(DP, "col", "row"), P(DP, "row", "col"), P(COL_DP, "row"))
    out_specs = (P(DP, "row", "col"), P(COL_DP, "row"))
    return jax.shard_map(on_device, mesh=split, in_specs=in_specs, out_specs=out_specs, check_vma=False)
```

```python
import jax
import jax.numpy as jnp
from jax import lax
from jax.sharding import Mesh
from jax.sharding import PartitionSpec as P

DP = ("z", "y")
COL_DP = ("col", "z", "y")


def crossed(value, by):
    cores = lax.axis_size("col")
    return lax.ppermute(value, "col", [(i, (i + by) % cores) for i in range(cores)])


def traded(value, axis, second):
    cores, devices = lax.axis_size("col"), lax.axis_size(axis)
    first = axis == "row"
    number = lambda c, place: (place + c) % devices * cores + c if first else c * devices + (place + c) % devices
    pairs = []
    for c in range(cores):
        for place in range(devices):
            other = place + (1 if (place % 2 == 0) != second else -1)
            pairs.append((number(c, place), number(c, other)))
    return lax.ppermute(value, (axis, "col") if first else ("col", axis), pairs)


def place_on(axis):
    return (lax.axis_index(axis) - lax.axis_index("col")) % lax.axis_size(axis)


def paired(own, other, odd):
    both = jnp.stack([own, other])
    return jnp.where(odd, both[::-1], both)


def gathered_pairs(value, axis):
    devices = lax.axis_size(axis)
    place = place_on(axis)
    odd, number = place % 2, place // 2
    ahead = 2 * odd - 1
    pair = paired(value, traded(value, axis, False), odd == 1)
    out = [(number, pair)]
    for step in range(2, devices // 2 + 1):
        pair = traded(pair, axis, step % 2 == 0)
        distance = step // 2 * (1 if step % 2 == 0 else -1)
        out.append(((number + ahead * distance) % (devices // 2), pair))
    return out


def around(axis):
    devices, index = lax.axis_size(axis), lax.axis_index(axis)
    ahead = 2 * (place_on(axis) % 2) - 1
    return [(index + 2) % devices, (index + ahead) % devices, (index - ahead) % devices, index]


def quartered(value, axis):
    beside = traded(value, axis, False)
    behind = traded(value, axis, True)
    return [traded(beside, axis, True), behind, beside, value]


def summed(part, axis):
    f32, bf16 = jnp.float32, jnp.bfloat16
    passed_on = traded(part(0).astype(bf16), axis, True)
    kept = traded(part(1).astype(bf16), axis, True)
    partners = part(2).astype(f32) + passed_on.astype(f32)
    came = traded(partners.astype(bf16), axis, False)
    return part(3).astype(f32) + kept.astype(f32) + came.astype(f32)


def on_device(out_grad, saved_hidden, down_weight):
    rows, cols, zs, ys = (lax.axis_size(a) for a in ("row", "col", "z", "y"))
    col = lax.axis_index("col")
    grad, hidden = out_grad[0], saved_hidden[0]
    units, width = down_weight.shape
    tokens, wide = hidden.shape
    block = ys * units
    f32, bf16 = jnp.float32, jnp.bfloat16

    parts = quartered(down_weight, "y")
    weight = jnp.zeros((block, width), down_weight.dtype)
    for index, part in zip(around("y"), parts):
        weight = lax.dynamic_update_slice(weight, part, (index * units, 0))

    mine = jnp.swapaxes(hidden.reshape(tokens, zs, block), 0, 1)
    mine = lax.all_to_all(mine, "z", 0, 0, tiled=True).reshape(zs * tokens, block)

    own = jnp.zeros((zs, *grad.shape), grad.dtype)
    for number, pair in gathered_pairs(grad, "z"):
        for n in range(2):
            own = lax.dynamic_update_slice(own, pair[n][None], ((2 * number + n + col) % zs, 0, 0))
    other = crossed(own, 1)
    per_core = rows // cols
    by_row = lambda v: jnp.swapaxes(v.reshape(zs, per_core, tokens, width), 0, 1)
    halves = jnp.concatenate([by_row(own), by_row(other)])
    grads = [
        lax.dynamic_index_in_dim(halves, (index - per_core * col) % rows, 0, keepdims=False).reshape(-1, width)
        for index in around("row")
    ]

    parts = quartered(mine, "row")
    hiddens = jnp.concatenate(parts)

    partial = lambda k: lax.dot_general(grads[k], weight, (((1,), (1,)), ((), ())), preferred_element_type=f32)
    local = summed(partial, "row").astype(bf16).reshape(zs, tokens, block)
    returned = lax.all_to_all(local, "z", 0, 0, tiled=True)
    hidden_grad = jnp.swapaxes(returned, 0, 1).reshape(1, tokens, wide)

    factor = f32(1.0) / jnp.sqrt(f32(rows * tokens * zs * ys))
    total = lax.dot_general(
        hiddens, jnp.concatenate(grads), (((0,), (0,)), ((), ())), preferred_element_type=f32
    ).astype(bf16)
    indices = around("y")
    take = lambda k: lax.dynamic_slice_in_dim(total, indices[k] * units, units, 0)
    weight_grad = (summed(take, "y") * factor).astype(bf16)
    return (hidden_grad, weight_grad)


def solution(mesh):
    dp = mesh.shape["dp"]
    split = Mesh(
        mesh.devices.reshape(mesh.shape["row"], mesh.shape["col"], 8, dp // 8),
        ("row", "col", "z", "y"),
    )
    in_specs = (P(DP, "col", "row"), P(DP, "row", "col"), P(COL_DP, "row"))
    out_specs = (P(DP, "row", "col"), P(COL_DP, "row"))
    return jax.shard_map(on_device, mesh=split, in_specs=in_specs, out_specs=out_specs, check_vma=False)
```

```python
import jax
import jax.numpy as jnp
from jax import lax
from jax.sharding import Mesh
from jax.sharding import PartitionSpec as P

DP = ("z", "y")
COL_DP = ("col", "z", "y")


def crossed(value, by):
    cores = lax.axis_size("col")
    return lax.ppermute(value, "col", [(i, (i + by) % cores) for i in range(cores)])


def traded(value, axis, second):
    cores, devices = lax.axis_size("col"), lax.axis_size(axis)
    first = axis == "row"
    number = lambda c, place: (place + c) % devices * cores + c if first else c * devices + (place + c) % devices
    pairs = []
    for c in range(cores):
        for place in range(devices):
            other = place + (1 if (place % 2 == 0) != second else -1)
            pairs.append((number(c, place), number(c, other)))
    return lax.ppermute(value, (axis, "col") if first else ("col", axis), pairs)


def place_on(axis):
    return (lax.axis_index(axis) - lax.axis_index("col")) % lax.axis_size(axis)


def paired(own, other, odd):
    both = jnp.stack([own, other])
    return jnp.where(odd, both[::-1], both)


def gathered_pairs(value, axis):
    devices = lax.axis_size(axis)
    place = place_on(axis)
    odd, number = place % 2, place // 2
    ahead = 2 * odd - 1
    pair = paired(value, traded(value, axis, False), odd == 1)
    out = [(number, pair)]
    for step in range(2, devices // 2 + 1):
        pair = traded(pair, axis, step % 2 == 0)
        distance = step // 2 * (1 if step % 2 == 0 else -1)
        out.append(((number + ahead * distance) % (devices // 2), pair))
    return out


def around(axis):
    devices, index = lax.axis_size(axis), lax.axis_index(axis)
    ahead = 2 * (place_on(axis) % 2) - 1
    return [(index + 2) % devices, (index + ahead) % devices, (index - ahead) % devices, index]


def quartered(value, axis):
    beside = traded(value, axis, False)
    behind = traded(value, axis, True)
    return [traded(beside, axis, True), behind, beside, value]


def summed(part, axis, early):
    f32, bf16 = jnp.float32, jnp.bfloat16
    first, second = part(0).astype(bf16), part(1).astype(bf16)
    third, fourth = part(2).astype(f32), part(3).astype(f32)
    if early:
        third, fourth = lax.optimization_barrier((third, fourth))
    passed_on = traded(first, axis, True)
    kept = traded(second, axis, True)
    partners = third + passed_on.astype(f32)
    came = traded(partners.astype(bf16), axis, False)
    return fourth + kept.astype(f32) + came.astype(f32)


def on_device(out_grad, saved_hidden, down_weight):
    rows, cols, zs, ys = (lax.axis_size(a) for a in ("row", "col", "z", "y"))
    col = lax.axis_index("col")
    grad, hidden = out_grad[0], saved_hidden[0]
    units, width = down_weight.shape
    tokens, wide = hidden.shape
    block = ys * units
    f32, bf16 = jnp.float32, jnp.bfloat16

    parts = quartered(down_weight, "y")
    weight = jnp.zeros((block, width), down_weight.dtype)
    for index, part in zip(around("y"), parts):
        weight = lax.dynamic_update_slice(weight, part, (index * units, 0))

    mine = jnp.swapaxes(hidden.reshape(tokens, zs, block), 0, 1)
    mine = lax.all_to_all(mine, "z", 0, 0, tiled=True).reshape(zs * tokens, block)

    own = jnp.zeros((zs, *grad.shape), grad.dtype)
    for number, pair in gathered_pairs(grad, "z"):
        for n in range(2):
            own = lax.dynamic_update_slice(own, pair[n][None], ((2 * number + n + col) % zs, 0, 0))
    other = crossed(own, 1)
    per_core = rows // cols
    by_row = lambda v: jnp.swapaxes(v.reshape(zs, per_core, tokens, width), 0, 1)
    halves = jnp.concatenate([by_row(own), by_row(other)])
    grads = [
        lax.dynamic_index_in_dim(halves, (index - per_core * col) % rows, 0, keepdims=False).reshape(-1, width)
        for index in around("row")
    ]

    parts = quartered(mine, "row")
    hiddens = jnp.concatenate(parts)

    partial = lambda k: lax.dot_general(grads[k], weight, (((1,), (1,)), ((), ())), preferred_element_type=f32)
    local = summed(partial, "row", True).astype(bf16).reshape(zs, tokens, block)
    returned = lax.all_to_all(local, "z", 0, 0, tiled=True)
    hidden_grad = jnp.swapaxes(returned, 0, 1).reshape(1, tokens, wide)

    factor = f32(1.0) / jnp.sqrt(f32(rows * tokens * zs * ys))
    total = lax.dot_general(
        hiddens, jnp.concatenate(grads), (((0,), (0,)), ((), ())), preferred_element_type=f32
    ).astype(bf16)
    indices = around("y")
    take = lambda k: lax.dynamic_slice_in_dim(total, indices[k] * units, units, 0)
    weight_grad = (summed(take, "y", False) * factor).astype(bf16)
    return (hidden_grad, weight_grad)


def solution(mesh):
    dp = mesh.shape["dp"]
    split = Mesh(
        mesh.devices.reshape(mesh.shape["row"], mesh.shape["col"], 8, dp // 8),
        ("row", "col", "z", "y"),
    )
    in_specs = (P(DP, "col", "row"), P(DP, "row", "col"), P(COL_DP, "row"))
    out_specs = (P(DP, "row", "col"), P(COL_DP, "row"))
    return jax.shard_map(on_device, mesh=split, in_specs=in_specs, out_specs=out_specs, check_vma=False)
```
